32 devices in a mesh: batch: 4 (over x, core), seq: 8 (over z, y).
Axes of the slice: x: 2, y: 2, z: 4, core: 2. Of those that a mesh axis runs over, the one named last changes fastest.
Arguments:
- query: bfloat16 [8, 64, 128], P('batch'), may hold values from -300 to 300
- cache_keys: bfloat16 [8, 16384, 512], P('batch', 'seq'), may hold values from -6 to 6
- cache_values: bfloat16 [8, 16384, 512], P('batch', 'seq'), may hold values from -6 to 6
- new_keys: bfloat16 [8, 512], P('batch'), may hold values from -6 to 6
- new_values: bfloat16 [8, 512], P('batch'), may hold values from -6 to 6
- key_up: bfloat16 [512, 1024], P('seq'), may hold values from -0.25 to 0.25
- value_up: bfloat16 [512, 1024], P('seq'), may hold values from -0.25 to 0.25
- out_weight: bfloat16 [8192, 8192], P('seq', 'batch'), may hold values from -0.5 to 0.5
- lengths: int32 [8], P('batch'), may hold values from 128 to 16384, as said below
Outputs:
- mixed: bfloat16 [8, 8192], P('seq', 'batch')
The draws below stay inside these ranges and needn't reach their ends.
Inputs may be any that keep to these rules, and one draw needn't show every extreme that they name: `lengths`: every length is a multiple of 128, at least 128; some sequence fills all 16384 slots. Slots at or beyond a sequence's length hold arbitrary finite entries that must not affect the result.
All inputs are finite; a program needn't handle non-finite values.
Results may differ from the reference program's by a relative error of at most 0.019.
Values may be sent and summed in bfloat16 or wider, within the bound.
A program may use at most 64 MiB of HBM per device.

```python
import jax
import jax.numpy as jnp
from jax import lax

D = 8192
H = 64
KV = 8
DH = 128
R = 512
BLOCK = 128
BATCH = 8
NTOK = 16384


def draw_query(key, part):
    base = jax.random.truncated_normal(key, -5.0, 5.0, (BATCH, H, DH), jnp.float32)
    values = base * 2.25
    return values.astype(jnp.bfloat16)


def draw_lengths(key, part):
    blocks = NTOK // BLOCK
    counts = jax.random.randint(key, (BATCH,), 1, blocks + 1)
    filled = jax.random.randint(jax.random.fold_in(key, 3), (), 0, BATCH)
    counts = jnp.where(jnp.arange(BATCH) == filled, blocks, counts)
    return (counts * BLOCK).astype(jnp.int32)


def level_of(rng, extent, shards, least, largest):
    factor_of, own = 1.0, jax.random.fold_in(rng, 6)
    for axis_at, blocks in shards:
        heights = jnp.exp(jax.random.uniform(jax.random.fold_in(own, axis_at), (blocks,), jnp.float32, least / len(shards), largest / len(shards)))
        factor_of = factor_of * jnp.repeat(heights, extent[axis_at] // blocks).reshape([-1 if axis == axis_at else 1 for axis in range(len(extent))])
    return factor_of


def noise(stream_key, dims, deviation, reach, shards=(), held_as=jnp.bfloat16):
    drawn = deviation * jax.random.normal(stream_key, dims, jnp.float32)
    if shards:
        drawn = drawn * level_of(stream_key, dims, shards, -0.22, 0.18)
    return jnp.clip(drawn, -reach, reach).astype(held_as)


def setup_inputs(seed: int = 0) -> dict:
    key_of = jax.random.split(jax.random.key(seed), 10)
    query = draw_query(jax.random.fold_in(key_of[9], 71), 0)
    cache_keys = noise(key_of[1], (BATCH, NTOK, R), 1.0, 6.0, ((0, 4), (1, 8)))
    cache_values = noise(key_of[2], (BATCH, NTOK, R), 1.0, 6.0, ((0, 4), (1, 8)))
    new_keys = noise(key_of[3], (BATCH, R), 1.0, 6.0, ((0, 4),))
    new_values = noise(key_of[4], (BATCH, R), 1.0, 6.0, ((0, 4),))
    key_up = noise(key_of[5], (R, KV * DH), R ** -0.5, 0.25, ((0, 8),))
    value_up = noise(key_of[6], (R, KV * DH), R ** -0.5, 0.25, ((0, 8),))
    out_weight = noise(key_of[7], (H * DH, D), DH ** -0.5, 0.5, ((0, 8), (1, 4)))
    lengths = draw_lengths(jax.random.fold_in(key_of[9], 71), 0)
    return dict(query=query, cache_keys=cache_keys, cache_values=cache_values, new_keys=new_keys, new_values=new_values, key_up=key_up, value_up=value_up, out_weight=out_weight, lengths=lengths)


def reference(query, cache_keys, cache_values, new_keys, new_values, key_up, value_up, out_weight, lengths):
    highest = lax.Precision.HIGHEST
    key_wide = key_up.astype(jnp.float32).reshape(R, KV, DH)
    value_wide = value_up.astype(jnp.float32).reshape(R, KV, DH)
    score_scale_factor = DH ** -0.5
    positions = jnp.arange(NTOK, dtype=jnp.int32)

    def per_sequence(items):
        query_row, keys_row, values_row, new_key_row, new_value_row, length = items
        grouped = query_row.astype(jnp.float32).reshape(KV, H // KV, DH)
        query_latent = jnp.einsum("kgd,rkd->kgr", grouped, key_wide, precision=highest)
        scores = jnp.einsum("kgr,lr->kgl", query_latent, keys_row.astype(jnp.float32), precision=highest) * score_scale_factor
        live_slots = positions < length
        scores = jnp.where(live_slots[None, None, :], scores, -jnp.inf)
        fresh_key_row = jnp.einsum("r,rkd->kd", new_key_row.astype(jnp.float32), key_wide, precision=highest)
        new_value = jnp.einsum("r,rkd->kd", new_value_row.astype(jnp.float32), value_wide, precision=highest)
        current_token_score = jnp.einsum("kgd,kd->kg", grouped, fresh_key_row, precision=highest) * score_scale_factor
        upper_limit = jnp.maximum(jnp.max(scores, axis=-1), current_token_score)
        softmax_terms = jnp.exp(scores - upper_limit[..., None])
        own_weight = jnp.exp(current_token_score - upper_limit)
        denominator = jnp.sum(softmax_terms, axis=-1) + own_weight
        latent_sum = jnp.einsum("kgl,lr->kgr", softmax_terms, values_row.astype(jnp.float32), precision=highest)
        totals = jnp.einsum("kgr,rkd->kgd", latent_sum, value_wide, precision=highest)
        totals = totals + own_weight[..., None] * new_value[:, None, :]
        return (totals / denominator[..., None]).reshape(H * DH).astype(jnp.bfloat16)

    attended = lax.map(per_sequence, (query, cache_keys, cache_values, new_keys, new_values, lengths))
    return jnp.dot(attended, out_weight, preferred_element_type=jnp.float32).astype(jnp.bfloat16)
```

```python
import functools

import jax
import jax.numpy as jnp
from jax import lax
from jax.experimental import pallas as pl
from jax.experimental.pallas import tpu as pltpu
from jax.sharding import PartitionSpec as P

NEGATIVE = -1e30
LOG2E = 1.4426950408889634
TOP_PRECISION = lax.Precision.HIGHEST
MESH = pl.DeviceIdType.MESH
NT = (((1,), (1,)), ((), ()))
NN = (((1,), (0,)), ((), ()))
F32 = jnp.float32
BF16 = jnp.bfloat16


def split_halves(x):
    head = x.astype(BF16)
    rest = (x - head.astype(F32)).astype(BF16)
    return jnp.concatenate([head, rest], axis=0)


def split_dot(x, y, dims):
    rows = x.shape[0]
    both = lax.dot_general(split_halves(x), y, dims, preferred_element_type=F32)
    return both[:rows] + both[rows:]


def dot(x, y, dims):
    return lax.dot_general(x, y, dims, preferred_element_type=F32)


def step_kernel(
    ns, nb, lengths, query, keys, values, new_k, new_v, key_up, value_up, out_w, out,
    kbuf, vbuf, wbuf, lens, qin, ku, vu, nk, nv, qbd, qs, rhs, score, turned_terms,
    vcol, os, orecv, stats, gains, att, attf, pscr, ps, pr,
    lsem, qsend, qrecv, vsend, vrecv, usend, urecv,
    ssend, srecv, osend, orcv, asend, arcv, psend, prcv,
):
    me = lax.axis_index("seq")
    mb = lax.axis_index("batch")
    seqs, heads, dh = qin.shape
    cache_len = kbuf.shape[1]
    rl, kv_width = ku.shape
    rank = kbuf.shape[2]
    hl = heads // ns
    kv = kv_width // dh
    group = heads // kv
    rows = seqs * hl
    lanes = seqs * heads
    quarter = rl // nb

    barrier = pltpu.get_barrier_semaphore()
    for d in range(1, ns):
        pl.semaphore_signal(
            barrier, inc=1, device_id={"seq": lax.rem(me + d, ns)}, device_id_type=MESH
        )
    for d in range(1, nb):
        pl.semaphore_signal(
            barrier, inc=1, device_id={"batch": lax.rem(mb + d, nb)}, device_id_type=MESH
        )

    local = [
        pltpu.make_async_copy(src, dst, lsem.at[i])
        for i, (src, dst) in enumerate(
            [
                (key_up, ku), (query, qin), (value_up, vu), (lengths, lens),
                (new_k, nk), (new_v, nv),
                (keys.at[0], kbuf.at[0]), (keys.at[1], kbuf.at[1]),
                (values.at[0], vbuf.at[0]), (values.at[1], vbuf.at[1]),
                (out_w, wbuf),
            ]
        )
    ]
    for copy in local:
        copy.start()

    started = []
    bits = [lax.rem(lax.div(me, 1 << i), 2) for i in range((ns - 1).bit_length())]

    def across(d):
        return sum((1 - x if d >> i & 1 else x) * (1 << i) for i, x in enumerate(bits))

    def turned(d):
        return lax.rem(mb + d, nb)

    def turned_back(d):
        return lax.rem(mb + nb - d, nb)

    def hop(src, dst, send, recv, d, axis, target):
        return pltpu.make_async_remote_copy(
            src_ref=src, dst_ref=dst, send_sem=send.at[d], recv_sem=recv.at[d],
            device_id={axis: target}, device_id_type=MESH,
        )

    def send_all(order, partner, index, axis, src_of, dst, send, recv):
        for d in order:
            copy = hop(src_of(partner(d)), dst(index), send, recv, d, axis, partner(d))
            copy.start()
            started.append(copy)

    def receive(d, partner, axis, src_of, dst, send, recv):
        hop(src_of(partner(d)), dst(partner(d)), send, recv, d, axis, partner(d)).wait_recv()

    near, far = list(range(1, ns // 2)), list(range(ns // 2, ns))
    everyone = far + near

    qbd[...] = jnp.zeros(qbd.shape, F32)
    local[0].wait()
    local[1].wait()
    for b in range(seqs):
        for k in range(kv):
            at = b * heads + k * group
            qbd[at : at + group, k * dh : (k + 1) * dh] = qin[
                b, k * group : (k + 1) * group, :
            ].astype(F32)
    asked = dot(ku[...], qbd[...].astype(BF16), NT) * (dh ** (-0.5) * LOG2E)
    qs[me] = asked
    local[2].wait()
    own_rows = pl.ds(pl.multiple_of(mb * quarter, quarter), quarter)
    own_column = pl.ds(pl.multiple_of(me * dh, 128), dh)
    vcol[me, mb] = vu[own_rows, own_column]

    pl.semaphore_wait(barrier, ns - 1 + nb - 1)

    q_args = (across, "seq", lambda t: qs.at[me], lambda s: qs.at[s], qsend, qrecv)
    v_args = (
        across, "seq",
        lambda t: vu.at[own_rows, pl.ds(pl.multiple_of(t * dh, 128), dh)],
        lambda s: vcol.at[s, mb],
        vsend, vrecv,
    )

    def post(order, args, index=me):
        partner, axis, src_of, dst, send, recv = args
        send_all(order, partner, index, axis, src_of, dst, send, recv)

    def take(order, args):
        for d in order:
            receive(d, *args)

    post(everyone, q_args)
    post(everyone, v_args)

    low = lax.broadcasted_iota(jnp.int32, (1, lanes), 1) < heads
    side = lax.div(me, ns // 2)
    half_rank = rank // 2

    def swap(x):
        return pltpu.roll(x, heads, 1)

    def gathered(half):
        for j in range(ns // 2):
            s = half * (ns // 2) + j
            x = qs[s]
            head = x.astype(BF16).astype(F32)
            rest = swap(x - head)
            span = pl.ds(pl.multiple_of(s * rl, rl), rl)
            rhs[0, span, :] = jnp.where(low, head, rest).astype(BF16)
            rhs[1, span, :] = jnp.where(low, rest, head).astype(BF16)

    chunk = 512
    spans = [slice(c, c + chunk) for c in range(0, cache_len, chunk)]

    def merged(r0, r1):
        return jnp.where(low, r0, r1) + swap(jnp.where(low, r1, r0))

    def half_scores(span, half):
        columns = pl.ds(pl.multiple_of(half * half_rank, 128), half_rank)
        return merged(
            *[dot(kbuf[b, span, columns], rhs[b, columns, :], NN) for b in range(seqs)]
        )

    take(near, q_args)
    gathered(side)
    for i in (6, 7, 3):
        local[i].wait()
    for span in spans:
        score[span, :] = half_scores(span, side)
    take(far, q_args)
    gathered(1 - side)

    limits = jnp.where(low, lens[0], lens[1]) - me * cache_len
    top = jnp.full((8, lanes), 0.5 * NEGATIVE, F32)
    for span in spans:
        positions = span.start + lax.broadcasted_iota(jnp.int32, (chunk, lanes), 0)
        whole = score[span, :] + half_scores(span, 1 - side)
        whole = jnp.where(positions < limits, whole, NEGATIVE)
        score[span, :] = whole
        top = jnp.maximum(top, jnp.max(whole.reshape(chunk // 8, 8, lanes), axis=0))
    top = jnp.max(top, axis=0, keepdims=True)

    local[8].wait()
    total = jnp.zeros((8, lanes), F32)
    sums = jnp.zeros((heads, rank), F32)
    for span in spans:
        terms = jnp.exp2(score[span, :] - top).astype(BF16)
        total = total + jnp.sum(terms.astype(F32).reshape(chunk // 8, 8, lanes), axis=0)
        across_lanes = terms.T
        turned_terms[:, span] = across_lanes[heads:, :]
        sums = sums + dot(across_lanes[:heads, :], vbuf[0, span, :], NN)
    stats[me, 0:1, :] = top
    stats[me, 1:2, :] = jnp.sum(total, axis=0, keepdims=True)
    s_args = (across, "seq", lambda t: stats.at[me], lambda s: stats.at[s], ssend, srecv)
    post(everyone, s_args)

    def o_args(b):
        return (
            across, "seq", lambda t: os.at[b, t], lambda s: orecv.at[b, s],
            osend.at[b], orcv.at[b],
        )

    def share(b, sums):
        for p in range(ns):
            os[b, p] = sums[p * hl : (p + 1) * hl].astype(BF16)
        post(everyone, o_args(b))
        orecv[b, me] = os[b, me]

    share(0, sums)
    take(everyone, v_args)
    u_args = (turned, "batch", lambda t: vcol.at[:, mb], lambda s: vcol.at[:, s], usend, urecv)
    post(range(1, nb), u_args, mb)
    local[9].wait()
    share(1, dot(turned_terms[...], vbuf[1], NN))

    local[4].wait()
    local[5].wait()
    fresh = [dot(nk[...], rhs[b], NN)[b : b + 1] for b in range(seqs)]
    own = merged(*[jnp.broadcast_to(x, (8, lanes)) for x in fresh])[0:1]

    take(everyone, s_args)
    tops, totals = stats[:, 0, :], stats[:, 1, :]
    limit = jnp.maximum(jnp.max(tops, axis=0, keepdims=True), own)
    factor = jnp.exp2(tops - limit)
    own_weight = jnp.exp2(own - limit)
    below = own_weight + jnp.sum(factor * totals, axis=0, keepdims=True)
    shares = jnp.concatenate(
        [factor / below, jnp.broadcast_to(own_weight / below, (lanes - ns, lanes))], axis=0
    )
    gains[...] = shares.T

    latents = []
    for b in range(seqs):
        gain = gains[pl.ds(pl.multiple_of(b * heads + me * hl, 8), hl), :]
        take(everyone, o_args(b))
        latent = gain[:, ns : ns + 1] * nv[b : b + 1, :].astype(F32)
        for p in range(ns):
            latent = latent + gain[:, p : p + 1] * orecv[b, p].astype(F32)
        latents.append(latent)
    latent = jnp.concatenate(latents, axis=0)
    for d in range(1, nb):
        receive(d, turned_back, *u_args[1:])
    attended = split_dot(latent, vcol[...].reshape(rank, dh), NN)
    att[mb] = attended.astype(BF16)

    a_args = (turned, "batch", lambda t: att.at[mb], lambda s: att.at[s], asend, arcv)
    post(range(1, nb), a_args, mb)
    local[10].wait()
    for d in range(1, nb):
        receive(d, turned_back, *a_args[1:])
    attf[...] = att[...].reshape(nb * rows, dh).astype(F32)
    features = jnp.concatenate(
        [attf[pl.ds(g, nb * seqs, stride=hl), :] for g in range(hl)], axis=1
    ).astype(BF16)
    product = dot(features, wbuf[...], NN)
    for j in range(pscr.shape[1]):
        pscr[:, j, :] = product[:, j * 128 : (j + 1) * 128]
    for p in range(ns):
        ps[p] = pscr[p].astype(BF16)
    p_args = (across, "seq", lambda t: ps.at[t], lambda s: pr.at[s], psend, prcv)
    post(everyone, p_args)
    pr[me] = ps[me]
    take(everyone, p_args)
    result = pr[0].astype(F32)
    for p in range(1, ns):
        result = result + pr[p].astype(F32)
    out[...] = result.astype(out.dtype)
    for copy in started:
        copy.wait_send()


def fused_body(
    query, cache_keys, cache_values, new_keys, new_values, key_up, value_up, out_weight, lengths
):
    ns, nb = lax.axis_size("seq"), lax.axis_size("batch")
    seqs, cache_len, rank = cache_keys.shape
    heads, dh = query.shape[1:]
    hl = heads // ns
    rl = key_up.shape[0]
    lanes = seqs * heads
    width = out_weight.shape[1]
    dma = pltpu.SemaphoreType.DMA
    vmem = pltpu.VMEM
    hbm = pl.BlockSpec(memory_space=pl.ANY)
    mixed = pl.pallas_call(
        functools.partial(step_kernel, ns, nb),
        out_shape=jax.ShapeDtypeStruct((width // 128, 128), BF16),
        in_specs=[hbm] * 9,
        out_specs=pl.BlockSpec(memory_space=pltpu.VMEM),
        scratch_shapes=[
            vmem(cache_keys.shape, BF16),
            vmem(cache_values.shape, BF16),
            vmem(out_weight.shape, BF16),
            pltpu.SMEM(lengths.shape, jnp.int32),
            vmem(query.shape, BF16),
            vmem(key_up.shape, BF16),
            vmem(value_up.shape, BF16),
            vmem(new_keys.shape, BF16),
            vmem(new_values.shape, BF16),
            vmem((lanes, key_up.shape[1]), F32),
            vmem((ns, rl, lanes), F32),
            vmem((seqs, rank, lanes), BF16),
            vmem((cache_len, lanes), F32),
            vmem((heads, cache_len), BF16),
            vmem((ns, nb, rl // nb, dh), BF16),
            vmem((seqs, ns, hl, rank), BF16),
            vmem((seqs, ns, hl, rank), BF16),
            vmem((ns, 2, lanes), F32),
            vmem((lanes, lanes), F32),
            vmem((nb, seqs * hl, dh), BF16),
            vmem((nb * seqs * hl, dh), F32),
            vmem((ns, width // 128, 128), F32),
            vmem((ns, width // 128, 128), BF16),
            vmem((ns, width // 128, 128), BF16),
            dma((11,)),
        ]
        + [dma((ns,))] * 4
        + [dma((nb,))] * 2
        + [dma((ns,))] * 2
        + [dma((seqs, ns))] * 2
        + [dma((nb,))] * 2
        + [dma((ns,))] * 2,
        compiler_params=pltpu.CompilerParams(collective_id=0, has_side_effects=True),
        name="decode_step",
    )(
        lengths, query, cache_keys, cache_values, new_keys, new_values, key_up, value_up, out_weight
    )
    return mixed.reshape(1, width)


def fits(mesh, query, cache_keys, key_up):
    ns, nb = mesh.shape["seq"], mesh.shape["batch"]
    heads, dh = query.shape[1:]
    kv = key_up.shape[1] // dh
    seqs = query.shape[0] // nb
    return (
        seqs == 2 and kv == ns and heads // kv == 8 and heads == 64 and dh == 128 and nb == 4
        and key_up.shape[0] // ns == 64 and query.shape[0] == ns
        and cache_keys.shape[1] // ns * cache_keys.shape[2] <= 2 ** 20
        and cache_keys.shape[1] // ns % 512 == 0
    )


def body(
    query, cache_keys, cache_values, new_keys, new_values, key_up, value_up, out_weight, lengths
):
    batch_rows, cache_len, rank_full = cache_keys.shape
    head_count, head_dimension = (query.shape[1], query.shape[2])
    kv_heads = key_up.shape[1] // head_dimension
    group_size = head_count // kv_heads
    score_scale_factor = head_dimension ** (-0.5)
    seq_index = lax.axis_index("seq")
    seq_count = lax.axis_size("seq")
    local_head_index = head_count // seq_count
    positions = seq_index * cache_len + lax.iota(jnp.int32, cache_len)
    live_mask = (positions[None, :] < lengths[:, None])[:, None, None, :]
    grouped = query.reshape(batch_rows, kv_heads, group_size, head_dimension)
    key_full, value_full = (
        lax.all_gather(key_up, "seq", axis=0, tiled=True),
        lax.all_gather(value_up, "seq", axis=0, tiled=True),
    )
    rebuilt_keys = jnp.dot(
        cache_keys.reshape(batch_rows * cache_len, rank_full),
        key_full,
        preferred_element_type=jnp.float32,
    ).reshape(batch_rows, cache_len, kv_heads, head_dimension)
    rebuilt_values = jnp.dot(
        cache_values.reshape(batch_rows * cache_len, rank_full),
        value_full,
        preferred_element_type=jnp.float32,
    ).reshape(batch_rows, cache_len, kv_heads, head_dimension)
    expanded_query = grouped.astype(jnp.float32)
    scores = (
        jnp.einsum("bkgd,blkd->bkgl", expanded_query, rebuilt_keys, precision=TOP_PRECISION)
        * score_scale_factor
    )
    fresh_key_row = jnp.dot(new_keys, key_full, preferred_element_type=jnp.float32).reshape(
        batch_rows, kv_heads, head_dimension
    )
    current_token_score = (
        jnp.einsum("phsu,phu->phs", expanded_query, fresh_key_row, precision=TOP_PRECISION)
        * score_scale_factor
    )
    new_value = jnp.dot(new_values, value_full, preferred_element_type=jnp.float32).reshape(
        batch_rows, kv_heads, head_dimension
    )
    scores = jnp.where(live_mask, scores, NEGATIVE)
    local_max = jnp.max(scores, axis=-1)
    upper_limit = jnp.maximum(lax.pmax(local_max, "seq"), current_token_score)
    softmax_terms = jnp.where(live_mask, jnp.exp(scores - upper_limit[..., None]), 0.0)
    denominator = jnp.sum(softmax_terms, axis=-1)
    totals = jnp.einsum("bkgl,blkd->bkgd", softmax_terms, rebuilt_values, precision=TOP_PRECISION)
    denominator, totals = (
        lax.psum(denominator.astype(jnp.bfloat16), "seq").astype(jnp.float32),
        lax.psum(totals.astype(jnp.bfloat16), "seq").astype(jnp.float32),
    )
    own_weight = jnp.exp(current_token_score - upper_limit)
    normalized = (totals + own_weight[..., None] * new_value[:, :, None, :]) / (
        denominator + own_weight
    )[..., None]
    normalized = normalized.reshape(batch_rows, head_count * head_dimension)
    width_local = local_head_index * head_dimension
    attended = lax.dynamic_slice_in_dim(normalized, seq_index * width_local, width_local, 1).astype(
        jnp.bfloat16
    )
    partial_out = jnp.dot(
        lax.all_gather(attended, "batch", axis=0, tiled=True),
        out_weight,
        preferred_element_type=jnp.float32,
    )
    return lax.psum_scatter(
        partial_out.astype(jnp.bfloat16), "seq", scatter_dimension=0, tiled=True
    )


def solution(mesh):
    placed = (
        P("batch", None, None),
        P("batch", "seq", None),
        P("batch", "seq", None),
        P("batch", None),
        P("batch", None),
        P("seq", None),
        P("seq", None),
        P("seq", "batch"),
        P("batch"),
    )

    def run(*args):
        chosen = fused_body if fits(mesh, args[0], args[1], args[5]) else body
        return jax.shard_map(
            chosen, mesh=mesh, in_specs=placed, out_specs=P("seq", "batch"), check_vma=False
        )(*args)

    return run
```

```python
import functools

import jax
import jax.numpy as jnp
from jax import lax
from jax.experimental import pallas as pl
from jax.experimental.pallas import tpu as pltpu
from jax.sharding import PartitionSpec as P

NEGATIVE = -1e30
LOG2E = 1.4426950408889634
TINY = 1e-30
CODES = 32767.0
TOP_PRECISION = lax.Precision.HIGHEST
MESH = pl.DeviceIdType.MESH
NT = (((1,), (1,)), ((), ()))
NN = (((1,), (0,)), ((), ()))
F32 = jnp.float32
BF16 = jnp.bfloat16


def split_halves(x):
    head = x.astype(BF16)
    rest = (x - head.astype(F32)).astype(BF16)
    return jnp.concatenate([head, rest], axis=0)


def split_dot(x, y, dims):
    rows = x.shape[0]
    both = lax.dot_general(split_halves(x), y, dims, preferred_element_type=F32)
    return both[:rows] + both[rows:]


def dot(x, y, dims):
    return lax.dot_general(x, y, dims, preferred_element_type=F32)


def step_kernel(
    ns, nb, lengths, query, keys, values, new_k, new_v, key_up, value_up, out_w, out,
    kbuf, vbuf, wbuf, lens, qin, ku, vu, nk, nv, qbd, qs, qscale, rhs, score, turned_terms,
    vcol, os, orecv, stats, gains, att, attf, pscr, ps, pr,
    lsem, qsend, qrecv, csend, crecv, vsend, vrecv, usend, urecv,
    ssend, srecv, osend, orcv, asend, arcv, psend, prcv,
):
    me = lax.axis_index("seq")
    mb = lax.axis_index("batch")
    seqs, heads, dh = qin.shape
    cache_len = kbuf.shape[1]
    rl, kv_width = ku.shape
    rank = kbuf.shape[2]
    hl = heads // ns
    kv = kv_width // dh
    group = heads // kv
    rows = seqs * hl
    lanes = seqs * heads
    quarter = rl // nb

    barrier = pltpu.get_barrier_semaphore()
    for d in range(1, ns):
        pl.semaphore_signal(
            barrier, inc=1, device_id={"seq": lax.rem(me + d, ns)}, device_id_type=MESH
        )
    for d in range(1, nb):
        pl.semaphore_signal(
            barrier, inc=1, device_id={"batch": lax.rem(mb + d, nb)}, device_id_type=MESH
        )

    local = [
        pltpu.make_async_copy(src, dst, lsem.at[i])
        for i, (src, dst) in enumerate(
            [
                (key_up, ku), (query, qin), (value_up, vu), (lengths, lens),
                (new_k, nk), (new_v, nv),
                (keys.at[0], kbuf.at[0]), (keys.at[1], kbuf.at[1]),
                (values.at[0], vbuf.at[0]), (values.at[1], vbuf.at[1]),
                (out_w, wbuf),
            ]
        )
    ]
    for copy in local:
        copy.start()

    started = []
    bits = [lax.rem(lax.div(me, 1 << i), 2) for i in range((ns - 1).bit_length())]

    def across(d):
        return sum((1 - x if d >> i & 1 else x) * (1 << i) for i, x in enumerate(bits))

    def turned(d):
        return lax.rem(mb + d, nb)

    def turned_back(d):
        return lax.rem(mb + nb - d, nb)

    def hop(src, dst, send, recv, d, axis, target):
        return pltpu.make_async_remote_copy(
            src_ref=src, dst_ref=dst, send_sem=send.at[d], recv_sem=recv.at[d],
            device_id={axis: target}, device_id_type=MESH,
        )

    def send_all(order, partner, index, axis, src_of, dst, send, recv):
        for d in order:
            copy = hop(src_of(partner(d)), dst(index), send, recv, d, axis, partner(d))
            copy.start()
            started.append(copy)

    def receive(d, partner, axis, src_of, dst, send, recv):
        hop(src_of(partner(d)), dst(partner(d)), send, recv, d, axis, partner(d)).wait_recv()

    near, far = list(range(1, ns // 2)), list(range(ns // 2, ns))
    everyone = far + near

    qbd[...] = jnp.zeros(qbd.shape, F32)
    local[0].wait()
    local[1].wait()
    for b in range(seqs):
        for k in range(kv):
            at = b * heads + k * group
            qbd[at : at + group, k * dh : (k + 1) * dh] = qin[
                b, k * group : (k + 1) * group, :
            ].astype(F32)
    asked = dot(ku[...], qbd[...].astype(BF16), NT) * (dh ** (-0.5) * LOG2E)
    largest = jnp.maximum(jnp.max(jnp.abs(asked), axis=0, keepdims=True), TINY)
    qscale[me] = largest * (1.0 / CODES)
    qs[me] = jnp.round(asked * (CODES / largest)).astype(jnp.int32).astype(jnp.int16)
    local[2].wait()
    own_rows = pl.ds(pl.multiple_of(mb * quarter, quarter), quarter)
    own_column = pl.ds(pl.multiple_of(me * dh, 128), dh)
    vcol[me, mb] = vu[own_rows, own_column]

    pl.semaphore_wait(barrier, ns - 1 + nb - 1)

    q_args = (across, "seq", lambda t: qs.at[me], lambda s: qs.at[s], qsend, qrecv)
    c_args = (across, "seq", lambda t: qscale.at[me], lambda s: qscale.at[s], csend, crecv)
    v_args = (
        across, "seq",
        lambda t: vu.at[own_rows, pl.ds(pl.multiple_of(t * dh, 128), dh)],
        lambda s: vcol.at[s, mb],
        vsend, vrecv,
    )

    def post(order, args, index=me):
        partner, axis, src_of, dst, send, recv = args
        send_all(order, partner, index, axis, src_of, dst, send, recv)

    def take(order, args):
        for d in order:
            receive(d, *args)

    post(everyone, c_args)
    post(everyone, q_args)
    post(everyone, v_args)

    low = lax.broadcasted_iota(jnp.int32, (1, lanes), 1) < heads
    side = lax.div(me, ns // 2)
    half_rank = rank // 2

    def swap(x):
        return pltpu.roll(x, heads, 1)

    def gathered(half):
        for j in range(ns // 2):
            s = half * (ns // 2) + j
            x = qs[s].astype(jnp.int32).astype(F32) * qscale[s]
            head = x.astype(BF16).astype(F32)
            rest = swap(x - head)
            span = pl.ds(pl.multiple_of(s * rl, rl), rl)
            rhs[0, span, :] = jnp.where(low, head, rest).astype(BF16)
            rhs[1, span, :] = jnp.where(low, rest, head).astype(BF16)

    chunk = 512
    spans = [slice(c, c + chunk) for c in range(0, cache_len, chunk)]

    def merged(r0, r1):
        return jnp.where(low, r0, r1) + swap(jnp.where(low, r1, r0))

    def half_scores(span, half):
        columns = pl.ds(pl.multiple_of(half * half_rank, 128), half_rank)
        return merged(
            *[dot(kbuf[b, span, columns], rhs[b, columns, :], NN) for b in range(seqs)]
        )

    take(near, q_args)
    take(near, c_args)
    gathered(side)
    for i in (6, 7, 3):
        local[i].wait()
    for span in spans:
        score[span, :] = half_scores(span, side)
    take(far, q_args)
    take(far, c_args)
    gathered(1 - side)

    limits = jnp.where(low, lens[0], lens[1]) - me * cache_len
    top = jnp.full((8, lanes), 0.5 * NEGATIVE, F32)
    for span in spans:
        positions = span.start + lax.broadcasted_iota(jnp.int32, (chunk, lanes), 0)
        whole = score[span, :] + half_scores(span, 1 - side)
        whole = jnp.where(positions < limits, whole, NEGATIVE)
        score[span, :] = whole
        top = jnp.maximum(top, jnp.max(whole.reshape(chunk // 8, 8, lanes), axis=0))
    top = jnp.max(top, axis=0, keepdims=True)

    local[8].wait()
    total = jnp.zeros((8, lanes), F32)
    sums = jnp.zeros((heads, rank), F32)
    for span in spans:
        terms = jnp.exp2(score[span, :] - top).astype(BF16)
        total = total + jnp.sum(terms.astype(F32).reshape(chunk // 8, 8, lanes), axis=0)
        across_lanes = terms.T
        turned_terms[:, span] = across_lanes[heads:, :]
        sums = sums + dot(across_lanes[:heads, :], vbuf[0, span, :], NN)
    stats[me, 0:1, :] = top
    stats[me, 1:2, :] = jnp.sum(total, axis=0, keepdims=True)
    s_args = (across, "seq", lambda t: stats.at[me], lambda s: stats.at[s], ssend, srecv)
    post(everyone, s_args)

    def o_args(b):
        return (
            across, "seq", lambda t: os.at[b, t], lambda s: orecv.at[b, s],
            osend.at[b], orcv.at[b],
        )

    def share(b, sums):
        for p in range(ns):
            os[b, p] = sums[p * hl : (p + 1) * hl].astype(BF16)
        post(everyone, o_args(b))
        orecv[b, me] = os[b, me]

    share(0, sums)
    take(everyone, v_args)
    u_args = (turned, "batch", lambda t: vcol.at[:, mb], lambda s: vcol.at[:, s], usend, urecv)
    post(range(1, nb), u_args, mb)
    local[9].wait()
    share(1, dot(turned_terms[...], vbuf[1], NN))

    local[4].wait()
    local[5].wait()
    fresh = [dot(nk[...], rhs[b], NN)[b : b + 1] for b in range(seqs)]
    own = merged(*[jnp.broadcast_to(x, (8, lanes)) for x in fresh])[0:1]

    take(everyone, s_args)
    tops, totals = stats[:, 0, :], stats[:, 1, :]
    limit = jnp.maximum(jnp.max(tops, axis=0, keepdims=True), own)
    factor = jnp.exp2(tops - limit)
    own_weight = jnp.exp2(own - limit)
    below = own_weight + jnp.sum(factor * totals, axis=0, keepdims=True)
    shares = jnp.concatenate(
        [factor / below, jnp.broadcast_to(own_weight / below, (lanes - ns, lanes))], axis=0
    )
    gains[...] = shares.T

    latents = []
    for b in range(seqs):
        gain = gains[pl.ds(pl.multiple_of(b * heads + me * hl, 8), hl), :]
        take(everyone, o_args(b))
        latent = gain[:, ns : ns + 1] * nv[b : b + 1, :].astype(F32)
        for p in range(ns):
            latent = latent + gain[:, p : p + 1] * orecv[b, p].astype(F32)
        latents.append(latent)
    latent = jnp.concatenate(latents, axis=0)
    for d in range(1, nb):
        receive(d, turned_back, *u_args[1:])
    attended = split_dot(latent, vcol[...].reshape(rank, dh), NN)
    att[mb] = attended.astype(BF16)

    a_args = (turned, "batch", lambda t: att.at[mb], lambda s: att.at[s], asend, arcv)
    post(range(1, nb), a_args, mb)
    local[10].wait()
    for d in range(1, nb):
        receive(d, turned_back, *a_args[1:])
    attf[...] = att[...].reshape(nb * rows, dh).astype(F32)
    features = jnp.concatenate(
        [attf[pl.ds(g, nb * seqs, stride=hl), :] for g in range(hl)], axis=1
    ).astype(BF16)
    product = dot(features, wbuf[...], NN)
    for j in range(pscr.shape[1]):
        pscr[:, j, :] = product[:, j * 128 : (j + 1) * 128]
    for p in range(ns):
        ps[p] = pscr[p].astype(BF16)
    p_args = (across, "seq", lambda t: ps.at[t], lambda s: pr.at[s], psend, prcv)
    post(everyone, p_args)
    pr[me] = ps[me]
    take(everyone, p_args)
    result = pr[0].astype(F32)
    for p in range(1, ns):
        result = result + pr[p].astype(F32)
    out[...] = result.astype(out.dtype)
    for copy in started:
        copy.wait_send()


def fused_body(
    query, cache_keys, cache_values, new_keys, new_values, key_up, value_up, out_weight, lengths
):
    ns, nb = lax.axis_size("seq"), lax.axis_size("batch")
    seqs, cache_len, rank = cache_keys.shape
    heads, dh = query.shape[1:]
    hl = heads // ns
    rl = key_up.shape[0]
    lanes = seqs * heads
    width = out_weight.shape[1]
    dma = pltpu.SemaphoreType.DMA
    vmem = pltpu.VMEM
    hbm = pl.BlockSpec(memory_space=pl.ANY)
    mixed = pl.pallas_call(
        functools.partial(step_kernel, ns, nb),
        out_shape=jax.ShapeDtypeStruct((width // 128, 128), BF16),
        in_specs=[hbm] * 9,
        out_specs=pl.BlockSpec(memory_space=pltpu.VMEM),
        scratch_shapes=[
            vmem(cache_keys.shape, BF16),
            vmem(cache_values.shape, BF16),
            vmem(out_weight.shape, BF16),
            pltpu.SMEM(lengths.shape, jnp.int32),
            vmem(query.shape, BF16),
            vmem(key_up.shape, BF16),
            vmem(value_up.shape, BF16),
            vmem(new_keys.shape, BF16),
            vmem(new_values.shape, BF16),
            vmem((lanes, key_up.shape[1]), F32),
            vmem((ns, rl, lanes), jnp.int16),
            vmem((ns, 1, lanes), F32),
            vmem((seqs, rank, lanes), BF16),
            vmem((cache_len, lanes), F32),
            vmem((heads, cache_len), BF16),
            vmem((ns, nb, rl // nb, dh), BF16),
            vmem((seqs, ns, hl, rank), BF16),
            vmem((seqs, ns, hl, rank), BF16),
            vmem((ns, 2, lanes), F32),
            vmem((lanes, lanes), F32),
            vmem((nb, seqs * hl, dh), BF16),
            vmem((nb * seqs * hl, dh), F32),
            vmem((ns, width // 128, 128), F32),
            vmem((ns, width // 128, 128), BF16),
            vmem((ns, width // 128, 128), BF16),
            dma((11,)),
        ]
        + [dma((ns,))] * 6
        + [dma((nb,))] * 2
        + [dma((ns,))] * 2
        + [dma((seqs, ns))] * 2
        + [dma((nb,))] * 2
        + [dma((ns,))] * 2,
        compiler_params=pltpu.CompilerParams(collective_id=0, has_side_effects=True),
        name="decode_step",
    )(
        lengths, query, cache_keys, cache_values, new_keys, new_values, key_up, value_up, out_weight
    )
    return mixed.reshape(1, width)


def fits(mesh, query, cache_keys, key_up):
    ns, nb = mesh.shape["seq"], mesh.shape["batch"]
    heads, dh = query.shape[1:]
    kv = key_up.shape[1] // dh
    seqs = query.shape[0] // nb
    return (
        seqs == 2 and kv == ns and heads // kv == 8 and heads == 64 and dh == 128 and nb == 4
        and key_up.shape[0] // ns == 64 and query.shape[0] == ns
        and cache_keys.shape[1] // ns * cache_keys.shape[2] <= 2 ** 20
        and cache_keys.shape[1] // ns % 512 == 0
    )


def body(
    query, cache_keys, cache_values, new_keys, new_values, key_up, value_up, out_weight, lengths
):
    batch_rows, cache_len, rank_full = cache_keys.shape
    head_count, head_dimension = (query.shape[1], query.shape[2])
    kv_heads = key_up.shape[1] // head_dimension
    group_size = head_count // kv_heads
    score_scale_factor = head_dimension ** (-0.5)
    seq_index = lax.axis_index("seq")
    seq_count = lax.axis_size("seq")
    local_head_index = head_count // seq_count
    positions = seq_index * cache_len + lax.iota(jnp.int32, cache_len)
    live_mask = (positions[None, :] < lengths[:, None])[:, None, None, :]
    grouped = query.reshape(batch_rows, kv_heads, group_size, head_dimension)
    key_full, value_full = (
        lax.all_gather(key_up, "seq", axis=0, tiled=True),
        lax.all_gather(value_up, "seq", axis=0, tiled=True),
    )
    rebuilt_keys = jnp.dot(
        cache_keys.reshape(batch_rows * cache_len, rank_full),
        key_full,
        preferred_element_type=jnp.float32,
    ).reshape(batch_rows, cache_len, kv_heads, head_dimension)
    rebuilt_values = jnp.dot(
        cache_values.reshape(batch_rows * cache_len, rank_full),
        value_full,
        preferred_element_type=jnp.float32,
    ).reshape(batch_rows, cache_len, kv_heads, head_dimension)
    expanded_query = grouped.astype(jnp.float32)
    scores = (
        jnp.einsum("bkgd,blkd->bkgl", expanded_query, rebuilt_keys, precision=TOP_PRECISION)
        * score_scale_factor
    )
    fresh_key_row = jnp.dot(new_keys, key_full, preferred_element_type=jnp.float32).reshape(
        batch_rows, kv_heads, head_dimension
    )
    current_token_score = (
        jnp.einsum("phsu,phu->phs", expanded_query, fresh_key_row, precision=TOP_PRECISION)
        * score_scale_factor
    )
    new_value = jnp.dot(new_values, value_full, preferred_element_type=jnp.float32).reshape(
        batch_rows, kv_heads, head_dimension
    )
    scores = jnp.where(live_mask, scores, NEGATIVE)
    local_max = jnp.max(scores, axis=-1)
    upper_limit = jnp.maximum(lax.pmax(local_max, "seq"), current_token_score)
    softmax_terms = jnp.where(live_mask, jnp.exp(scores - upper_limit[..., None]), 0.0)
    denominator = jnp.sum(softmax_terms, axis=-1)
    totals = jnp.einsum("bkgl,blkd->bkgd", softmax_terms, rebuilt_values, precision=TOP_PRECISION)
    denominator, totals = (
        lax.psum(denominator.astype(jnp.bfloat16), "seq").astype(jnp.float32),
        lax.psum(totals.astype(jnp.bfloat16), "seq").astype(jnp.float32),
    )
    own_weight = jnp.exp(current_token_score - upper_limit)
    normalized = (totals + own_weight[..., None] * new_value[:, :, None, :]) / (
        denominator + own_weight
    )[..., None]
    normalized = normalized.reshape(batch_rows, head_count * head_dimension)
    width_local = local_head_index * head_dimension
    attended = lax.dynamic_slice_in_dim(normalized, seq_index * width_local, width_local, 1).astype(
        jnp.bfloat16
    )
    partial_out = jnp.dot(
        lax.all_gather(attended, "batch", axis=0, tiled=True),
        out_weight,
        preferred_element_type=jnp.float32,
    )
    return lax.psum_scatter(
        partial_out.astype(jnp.bfloat16), "seq", scatter_dimension=0, tiled=True
    )


def solution(mesh):
    placed = (
        P("batch", None, None),
        P("batch", "seq", None),
        P("batch", "seq", None),
        P("batch", None),
        P("batch", None),
        P("seq", None),
        P("seq", None),
        P("seq", "batch"),
        P("batch"),
    )

    def run(*args):
        chosen = fused_body if fits(mesh, args[0], args[1], args[5]) else body
        return jax.shard_map(
            chosen, mesh=mesh, in_specs=placed, out_specs=P("seq", "batch"), check_vma=False
        )(*args)

    return run
```
